16 devices in a mesh: dp: 2 (over y, z), ep: 8 (over x, core).
Axes of the slice: x: 4, y: 2, z: 1, core: 2. Of those that a mesh axis runs over, the one named last changes fastest.
The devices are a block of a 4x4x8 slice.
Arguments:
- tokens: bfloat16 [8192, 2048], P(('dp', 'ep')), parts along dimension 0
- expert_ids: int32 [8192, 6], P(('dp', 'ep')), parts along dimension 0
- gate_vals: float32 [8192, 6], P(('dp', 'ep')), parts along dimension 0
- slots: int32 [8192, 6], P(('dp', 'ep')), parts along dimension 0
- shared_w1: bfloat16 [2048, 2816], replicated
- shared_w3: bfloat16 [2048, 2816], replicated
- shared_w2: bfloat16 [2816, 2048], replicated
- shared_gate: bfloat16 [2048], replicated
- expert_w1: bfloat16 [64, 2048, 1408], P('ep')
- expert_w3: bfloat16 [64, 2048, 1408], P('ep')
- expert_w2: bfloat16 [64, 1408, 2048], P('ep')
Outputs:
- output: bfloat16 [8192, 2048], P(('dp', 'ep')), parts along dimension 0
There are 2 independent parts. The reference program is written for one: setup_inputs(seed, part) draws one part's arguments, and reference() takes and returns one part's arrays. A program takes and returns all parts, laid end to end along the dimension named above; an argument that names none is the same for every part.
All inputs are finite; a program needn't handle non-finite values.
Results may differ from the reference program's by a relative error of at most 0.00518217.
Values are sent between devices in bfloat16 or wider.
A program may use at most 768 MiB of HBM per device.

```python
import jax
import jax.numpy as jnp
from jax import lax

EP_SIZE = 8
TOKENS_DEV = 512
HIDDEN = 2048
EXPERTS = 64
TOP_K = 6
EXPERT_FF = 1408
SHARED_FF = 2816
CAPACITY = 96

NUM_TOKENS = EP_SIZE * TOKENS_DEV
BUF_ROWS = EXPERTS * CAPACITY


def draw_routes(route_key):
    score_key, bias_key, hot_key = jax.random.split(route_key, 3)
    scores = jax.random.randint(score_key, (NUM_TOKENS, EXPERTS), 0, 4096)
    expert_bias = jax.random.randint(bias_key, (EXPERTS,), 0, 1024)
    hot_expert = jax.random.randint(hot_key, (), 0, EXPERTS)
    expert_pos = jnp.arange(EXPERTS)
    forced = ((jnp.arange(NUM_TOKENS) % 2) == 0)[:, None] & (expert_pos[None, :] == hot_expert)
    total_score = scores + expert_bias[None, :] + jnp.where(forced, 8192, 0)
    distinct = total_score * EXPERTS + expert_pos[None, :]
    return lax.top_k(distinct, TOP_K)[1].astype(jnp.int32)


def source_slots(src_ids):
    flat_ids = src_ids.reshape(TOKENS_DEV * TOP_K)
    one_hot = (flat_ids[:, None] == jnp.arange(EXPERTS)[None, :]).astype(jnp.int32)
    earlier = jnp.cumsum(one_hot, axis=0) - one_hot
    position = jnp.sum(earlier * one_hot, axis=1)
    return jnp.where(position < CAPACITY, position, -1).reshape(TOKENS_DEV, TOP_K).astype(jnp.int32)


def normal_stack(stack_key, rows, cols):
    def one_matrix(one_key):
        return (jax.random.normal(one_key, (rows, cols), jnp.float32) * rows ** -0.5).astype(jnp.bfloat16)
    return lax.map(one_matrix, jax.random.split(stack_key, EXPERTS))


def setup_inputs(seed: int = 0, part: int = 0) -> dict:
    part_key = jax.random.fold_in(jax.random.key(seed), part)
    tok_key, route_key, gate_key = jax.random.split(part_key, 3)
    weight_keys = jax.random.split(jax.random.key(seed + 1), 7)
    tokens = jax.random.normal(tok_key, (NUM_TOKENS, HIDDEN), jnp.float32).astype(jnp.bfloat16)
    expert_ids = draw_routes(route_key)
    slots = lax.map(source_slots, expert_ids.reshape(EP_SIZE, TOKENS_DEV, TOP_K)).reshape(NUM_TOKENS, TOP_K)
    gate_vals = jax.random.uniform(gate_key, (NUM_TOKENS, TOP_K), jnp.float32, 0.5, 1.5) * TOP_K ** -0.5
    shared_w1 = (jax.random.normal(weight_keys[0], (HIDDEN, SHARED_FF), jnp.float32) * HIDDEN ** -0.5).astype(jnp.bfloat16)
    shared_w3 = (jax.random.normal(weight_keys[1], (HIDDEN, SHARED_FF), jnp.float32) * HIDDEN ** -0.5).astype(jnp.bfloat16)
    shared_w2 = (jax.random.normal(weight_keys[2], (SHARED_FF, HIDDEN), jnp.float32) * SHARED_FF ** -0.5).astype(jnp.bfloat16)
    shared_gate = (jax.random.normal(weight_keys[3], (HIDDEN,), jnp.float32) * 2.0 * HIDDEN ** -0.5).astype(jnp.bfloat16)
    expert_w1 = normal_stack(weight_keys[4], HIDDEN, EXPERT_FF)
    expert_w3 = normal_stack(weight_keys[5], HIDDEN, EXPERT_FF)
    expert_w2 = normal_stack(weight_keys[6], EXPERT_FF, HIDDEN)
    return {'tokens': tokens, 'expert_ids': expert_ids, 'gate_vals': gate_vals, 'slots': slots, 'shared_w1': shared_w1, 'shared_w3': shared_w3, 'shared_w2': shared_w2, 'shared_gate': shared_gate, 'expert_w1': expert_w1, 'expert_w3': expert_w3, 'expert_w2': expert_w2}


def swiglu_rows(rows, w_up, w_in, w_down):
    act_a = jnp.dot(rows, w_up, preferred_element_type=jnp.float32)
    act_b = jnp.dot(rows, w_in, preferred_element_type=jnp.float32)
    hidden_act = (jax.nn.silu(act_a) * act_b).astype(jnp.bfloat16)
    return jnp.dot(hidden_act, w_down, preferred_element_type=jnp.float32)


def reference(tokens, expert_ids, gate_vals, slots, shared_w1, shared_w3, shared_w2, shared_gate, expert_w1, expert_w3, expert_w2):
    src_tokens = tokens.reshape(EP_SIZE, TOKENS_DEV, HIDDEN)
    kept_mask = slots >= 0
    slot_dest = jnp.where(kept_mask, expert_ids * CAPACITY + slots, BUF_ROWS)
    flat_dest = slot_dest.reshape(EP_SIZE, TOKENS_DEV * TOP_K)
    copy_tok = jnp.arange(TOKENS_DEV * TOP_K, dtype=jnp.int32) // TOP_K

    def dispatch_one(operands):
        src_rows, src_dest = operands
        row_owner = jnp.full((BUF_ROWS + 1,), TOKENS_DEV, jnp.int32).at[src_dest].set(copy_tok)
        return jnp.take(src_rows, row_owner[:BUF_ROWS], axis=0, mode='fill', fill_value=0)

    buffers = lax.map(dispatch_one, (src_tokens, flat_dest))
    per_expert = buffers.reshape(EP_SIZE, EXPERTS, CAPACITY, HIDDEN).transpose(1, 0, 2, 3).reshape(EXPERTS, EP_SIZE * CAPACITY, HIDDEN)

    def expert_one(operands):
        rows, w_up, w_in, w_down = operands
        return swiglu_rows(rows, w_up, w_in, w_down).astype(jnp.bfloat16)

    expert_out = lax.map(expert_one, (per_expert, expert_w1, expert_w3, expert_w2))
    returned = expert_out.reshape(EXPERTS, EP_SIZE, CAPACITY, HIDDEN).transpose(1, 0, 2, 3).reshape(EP_SIZE, BUF_ROWS, HIDDEN)
    weights = jnp.where(kept_mask, gate_vals, 0.0).reshape(EP_SIZE, TOKENS_DEV, TOP_K)
    src_dest = slot_dest.reshape(EP_SIZE, TOKENS_DEV, TOP_K)

    def combine_one(operands):
        src_rows, src_out, src_idx, src_weights = operands
        picked = jnp.take(src_out, src_idx, axis=0, mode='fill', fill_value=0)
        routed = jnp.einsum('tk,tkd->td', src_weights, picked.astype(jnp.float32))
        gate_logit = jnp.dot(src_rows, shared_gate, preferred_element_type=jnp.float32)
        shared_out = jax.nn.sigmoid(gate_logit)[:, None] * swiglu_rows(src_rows, shared_w1, shared_w3, shared_w2)
        return (src_rows.astype(jnp.float32) + shared_out + routed).astype(jnp.bfloat16)

    result = lax.map(combine_one, (src_tokens, returned, src_dest, weights))
    return result.reshape(NUM_TOKENS, HIDDEN)
```

```python
import functools

import jax
import jax.numpy as jnp
from jax import lax
from jax.experimental import pallas as pl
from jax.experimental.pallas import tpu as pltpu
from jax.sharding import PartitionSpec as P

LANES = 128
TILE = 128
LOW = 32
VMEM_BYTES = 67043328


def chunk_sizes(tok_count):
    quarter = tok_count // 4
    return (quarter, quarter, quarter, quarter)


def router_kernel(sizes, top_k, meta_ref, me_ref, tok_ref, gate_ref, cnt_ref, rank_ref, g_ref):
    num_src = meta_ref.shape[0]
    num_e = rank_ref.shape[0]
    highs = tok_ref.shape[2]
    first = (me_ref[0] * num_e).astype(jnp.float32)
    e_idx = lax.broadcasted_iota(jnp.int32, (num_e, LANES), 0).astype(jnp.float32) + first
    upper = (lax.broadcasted_iota(jnp.int32, (LANES, LANES), 0)
             < lax.broadcasted_iota(jnp.int32, (LANES, LANES), 1)).astype(jnp.float32).astype(jnp.bfloat16)
    start = 0
    for c, size in enumerate(sizes):
        total = num_src * size
        carry = jnp.zeros((num_e, 1), jnp.float32)
        for s in range(num_src):
            for b in range(size // LANES):
                lane0 = start + b * LANES
                mask = jnp.zeros((num_e, LANES), jnp.float32)
                gate = jnp.zeros((num_e, LANES), jnp.float32)
                for k in range(top_k):
                    hit = meta_ref[s, k:k + 1, lane0:lane0 + LANES] == e_idx
                    mask = mask + jnp.where(hit, 1.0, 0.0)
                    gate = gate + jnp.where(hit, meta_ref[s, top_k + k:top_k + k + 1, lane0:lane0 + LANES], 0.0)
                rank = jnp.dot(mask.astype(jnp.bfloat16), upper, preferred_element_type=jnp.float32) + carry
                carry = carry + jnp.sum(mask, axis=1, keepdims=True)
                col = s * size + b * LANES
                rank_ref[:, col:col + LANES] = jnp.where(mask > 0.5, rank, -1.0)
                g_ref[:, col:col + LANES] = gate
        cnt_ref[c] = jnp.broadcast_to(carry, (num_e, LANES)).astype(jnp.int32)
        pos = lax.broadcasted_iota(jnp.int32, (1, total), 1)
        pos_hi = (pos // 64).astype(jnp.float32)
        pos_lo = (pos % 64).astype(jnp.float32)
        hi_iota = lax.broadcasted_iota(jnp.int32, (highs, total), 0).astype(jnp.float32)
        lo_iota = lax.broadcasted_iota(jnp.int32, (LOW, total), 0).astype(jnp.float32)
        slot_iota = (lax.broadcasted_iota(jnp.int32, (highs, LOW), 0) * LOW
                     + lax.broadcasted_iota(jnp.int32, (highs, LOW), 1)).astype(jnp.float32)
        for e in range(num_e):
            rank = rank_ref[e:e + 1, 0:total]
            gate = g_ref[e:e + 1, 0:total]
            hi = jnp.floor(rank * (1.0 / LOW))
            lo = rank - hi * LOW
            in_hi = hi_iota == hi
            in_lo = (lo_iota == lo).astype(jnp.float32).astype(jnp.bfloat16)
            gate_a = gate.astype(jnp.bfloat16).astype(jnp.float32)
            rest = gate - gate_a
            gate_b = rest.astype(jnp.bfloat16).astype(jnp.float32)
            gate_c = rest - gate_b
            left = jnp.concatenate(
                [jnp.where(in_hi, v, 0.0) for v in (pos_hi, pos_lo, gate_a, gate_b, gate_c)], axis=0)
            table = lax.dot_general(left.astype(jnp.bfloat16), in_lo, (((1,), (1,)), ((), ())),
                                    preferred_element_type=jnp.float32)
            tok = table[0:highs] * 64.0 + table[highs:2 * highs]
            live = slot_iota < carry[e:e + 1, 0:1]
            tok_ref[c, e] = jnp.where(live, tok, float(total)).astype(jnp.int32)
            gate_ref[c, e] = table[2 * highs:3 * highs] + (table[3 * highs:4 * highs] + table[4 * highs:5 * highs])
        start += size


def route(meta_all, me, sizes, top_k, num_e, rows_max):
    num_src = meta_all.shape[0]
    n_chunks = len(sizes)
    highs = rows_max // LOW
    width = num_src * max(sizes)
    tok, gate, cnt = pl.pallas_call(
        functools.partial(router_kernel, sizes, top_k),
        out_shape=(jax.ShapeDtypeStruct((n_chunks, num_e, highs, LOW), jnp.int32),
                   jax.ShapeDtypeStruct((n_chunks, num_e, highs, LOW), jnp.float32),
                   jax.ShapeDtypeStruct((n_chunks, num_e, LANES), jnp.int32)),
        in_specs=[pl.BlockSpec(memory_space=pltpu.VMEM), pl.BlockSpec(memory_space=pltpu.SMEM)],
        out_specs=(pl.BlockSpec(memory_space=pltpu.VMEM),) * 3,
        scratch_shapes=[pltpu.VMEM((num_e, width), jnp.float32), pltpu.VMEM((num_e, width), jnp.float32)],
        compiler_params=pltpu.CompilerParams(vmem_limit_bytes=32 * 1024 * 1024),
        name="router",
    )(meta_all, me)
    return (tok.reshape(n_chunks, num_e, rows_max), gate.reshape(n_chunks, num_e, rows_max), cnt[:, :, 0])


def ffn_kernel(cnt_ref, tok_ref, gate_ref, x_hbm, w1_ref, w3_ref, w2_ref, out_hbm,
               stage, xf, yf, xg, hb, rg, in_sem, out_sem):
    e = pl.program_id(0)
    num_e = pl.num_programs(0)
    rows, hidden = x_hbm.shape
    ff = w1_ref.shape[2]
    piece = stage.shape[1]
    pieces = rows // piece

    @pl.when(e == 0)
    def _():
        def fetch(i, slot):
            return pltpu.make_async_copy(x_hbm.at[pl.ds(i * piece, piece), :], stage.at[slot], in_sem.at[slot])
        fetch(0, 0).start()
        for i in range(pieces):
            if i + 1 < pieces:
                fetch(i + 1, (i + 1) % 2).start()
            fetch(i, i % 2).wait()
            xf[i * piece:(i + 1) * piece, :] = stage[i % 2].astype(jnp.float32)
            yf[i * piece:(i + 1) * piece, :] = jnp.zeros((piece, hidden), jnp.float32)
        xf[rows:rows + 8, :] = jnp.zeros((8, hidden), jnp.float32)
        yf[rows:rows + 8, :] = jnp.zeros((8, hidden), jnp.float32)

    count = cnt_ref[e]

    def one_tile(i, carry):
        base = i * TILE
        groups = (jnp.minimum(count - base, TILE) + 7) // 8

        def gather(j, c):
            for r in range(8):
                tok = tok_ref[e, base + j * 8 + r]
                xg[pl.ds(j * 8 + r, 1), :] = xf[pl.ds(tok, 1), :]
            return c
        lax.fori_loop(0, groups, gather, 0)
        x = xg[...].astype(jnp.bfloat16)
        for f in range(0, ff, 256):
            g = min(f + 256, ff)
            a = jnp.dot(x, w1_ref[0, :, f:g], preferred_element_type=jnp.float32)
            b = jnp.dot(x, w3_ref[0, :, f:g], preferred_element_type=jnp.float32)
            hb[:, f:g] = (jax.nn.silu(a) * b).astype(jnp.bfloat16)
        h = hb[...]
        for d in range(0, hidden, 512):
            r = jnp.dot(h, w2_ref[0, :, d:d + 512], preferred_element_type=jnp.float32)
            rg[:, d:d + 512] = r.astype(jnp.bfloat16).astype(jnp.float32)

        def combine(j, c):
            toks = [tok_ref[e, base + j * 8 + r] for r in range(8)]
            gates = [gate_ref[e, base + j * 8 + r] for r in range(8)]
            old = [yf[pl.ds(toks[r], 1), :] for r in range(8)]
            new = [old[r] + gates[r] * rg[pl.ds(j * 8 + r, 1), :] for r in range(8)]
            for r in range(8):
                yf[pl.ds(toks[r], 1), :] = new[r]
            return c
        lax.fori_loop(0, groups, combine, 0)
        return carry

    lax.fori_loop(0, (count + TILE - 1) // TILE, one_tile, 0)

    @pl.when(e == num_e - 1)
    def _():
        copy = pltpu.make_async_copy(yf.at[pl.ds(0, rows), :], out_hbm, out_sem)
        copy.start()
        copy.wait()


def expert_ffn(cnt, tok, gate, x, w1, w3, w2):
    rows, hidden = x.shape
    num_e, _, ff = w1.shape
    piece = 128
    return pl.pallas_call(
        ffn_kernel,
        out_shape=jax.ShapeDtypeStruct((rows, hidden), jnp.float32),
        grid_spec=pltpu.PrefetchScalarGridSpec(
            num_scalar_prefetch=3,
            grid=(num_e,),
            in_specs=[pl.BlockSpec(memory_space=pl.ANY),
                      pl.BlockSpec((1, hidden, ff), lambda e, *_: (e, 0, 0)),
                      pl.BlockSpec((1, hidden, ff), lambda e, *_: (e, 0, 0)),
                      pl.BlockSpec((1, ff, hidden), lambda e, *_: (e, 0, 0))],
            out_specs=pl.BlockSpec(memory_space=pl.ANY),
            scratch_shapes=[pltpu.VMEM((2, piece, hidden), jnp.bfloat16),
                            pltpu.VMEM((rows + 8, hidden), jnp.float32),
                            pltpu.VMEM((rows + 8, hidden), jnp.float32),
                            pltpu.VMEM((TILE, hidden), jnp.float32),
                            pltpu.VMEM((TILE, ff), jnp.bfloat16),
                            pltpu.VMEM((TILE, hidden), jnp.float32),
                            pltpu.SemaphoreType.DMA((2,)),
                            pltpu.SemaphoreType.DMA],
        ),
        compiler_params=pltpu.CompilerParams(vmem_limit_bytes=VMEM_BYTES),
        cost_estimate=pl.CostEstimate(flops=6 * rows * hidden * ff, bytes_accessed=6 * num_e * hidden * ff,
                                      transcendentals=0),
        name="expert_ffn",
    )(cnt, tok, gate, x, w1, w3, w2)


def solution(mesh):
    num_ep = mesh.shape['ep']
    row_spec = P(('dp', 'ep'), None)
    replicated = P()
    expert_spec = P('ep', None, None)

    def device_step(tokens, expert_ids, gate_vals, slots, shared_w1, shared_w3, shared_w2, shared_gate, expert_w1, expert_w3, expert_w2):
        tok_count, hidden = tokens.shape
        top_k = expert_ids.shape[1]
        num_e = expert_w1.shape[0]
        num_experts = num_e * num_ep
        capacity = 8 * ((2 * tok_count * top_k + 8 * num_experts - 1) // (8 * num_experts))
        rows_max = num_ep * capacity
        sizes = chunk_sizes(tok_count)
        me = lax.axis_index('ep').astype(jnp.int32).reshape(1)

        kept_ids = jnp.where(slots >= 0, expert_ids, -1).astype(jnp.float32)
        meta = jnp.concatenate([kept_ids, gate_vals], axis=1).T
        meta = jnp.pad(meta, ((0, -meta.shape[0] % 8), (0, 0)))
        meta_all = lax.all_gather(meta, 'ep', axis=0, tiled=False)
        tok, gate, cnt = route(meta_all, me, sizes, top_k, num_e, rows_max)

        start = 0
        gathered = []
        for size in sizes:
            x = lax.all_gather(tokens[start:start + size], 'ep', axis=0, tiled=False)
            gathered.append(x.reshape(num_ep * size, hidden))
            start += size

        gate_logit = jnp.dot(tokens, shared_gate, preferred_element_type=jnp.float32)
        shared_a = jnp.dot(tokens, shared_w1, preferred_element_type=jnp.float32)
        shared_b = jnp.dot(tokens, shared_w3, preferred_element_type=jnp.float32)
        shared_h = (jax.nn.silu(shared_a) * shared_b).astype(jnp.bfloat16)
        shared_out = jnp.dot(shared_h, shared_w2, preferred_element_type=jnp.float32)
        base = tokens.astype(jnp.float32) + jax.nn.sigmoid(gate_logit)[:, None] * shared_out

        parts = []
        start = 0
        for c, size in enumerate(sizes):
            partial = expert_ffn(cnt[c], tok[c], gate[c], gathered[c], expert_w1, expert_w3, expert_w2)
            routed = lax.psum_scatter(partial.reshape(num_ep, size, hidden), 'ep', scatter_dimension=0, tiled=False)
            parts.append((base[start:start + size] + routed).astype(jnp.bfloat16))
            start += size
        return jnp.concatenate(parts, axis=0)

    return jax.shard_map(device_step, mesh=mesh, in_specs=(row_spec, row_spec, row_spec, row_spec, replicated, replicated, replicated, replicated, expert_spec, expert_spec, expert_spec), out_specs=row_spec, check_vma=False)
```

```python
import functools

import jax
import jax.numpy as jnp
from jax import lax
from jax.experimental import pallas as pl
from jax.experimental.pallas import tpu as pltpu
from jax.sharding import PartitionSpec as P

LANES = 128
STEP = 64
TILE = 128
LOW = 32
VMEM_BYTES = 67043328


def chunk_sizes(tok_count):
    quarter = tok_count // 4
    rest = (tok_count - quarter) // 2
    return (quarter, rest, rest)


def router_kernel(sizes, top_k, meta_ref, me_ref, tok_ref, gate_ref, cnt_ref, rank_ref, g_ref):
    num_src = meta_ref.shape[0]
    num_e = rank_ref.shape[0]
    highs = tok_ref.shape[2]
    first = (me_ref[0] * num_e).astype(jnp.float32)
    e_idx = lax.broadcasted_iota(jnp.int32, (num_e, STEP), 0).astype(jnp.float32) + first
    upper = (lax.broadcasted_iota(jnp.int32, (STEP, STEP), 0)
             < lax.broadcasted_iota(jnp.int32, (STEP, STEP), 1)).astype(jnp.float32).astype(jnp.bfloat16)
    start = 0
    for c, size in enumerate(sizes):
        total = num_src * size
        carry = jnp.zeros((num_e, 1), jnp.float32)
        for s in range(num_src):
            for b in range(size // STEP):
                lane0 = start + b * STEP
                mask = jnp.zeros((num_e, STEP), jnp.float32)
                gate = jnp.zeros((num_e, STEP), jnp.float32)
                for k in range(top_k):
                    hit = meta_ref[s, k:k + 1, lane0:lane0 + STEP] == e_idx
                    mask = mask + jnp.where(hit, 1.0, 0.0)
                    gate = gate + jnp.where(hit, meta_ref[s, top_k + k:top_k + k + 1, lane0:lane0 + STEP], 0.0)
                rank = jnp.dot(mask.astype(jnp.bfloat16), upper, preferred_element_type=jnp.float32) + carry
                carry = carry + jnp.sum(mask, axis=1, keepdims=True)
                col = s * size + b * STEP
                rank_ref[:, col:col + STEP] = jnp.where(mask > 0.5, rank, -1.0)
                g_ref[:, col:col + STEP] = gate
        cnt_ref[c] = jnp.broadcast_to(carry, (num_e, LANES)).astype(jnp.int32)
        pos = lax.broadcasted_iota(jnp.int32, (1, total), 1)
        pos_hi = (pos // 64).astype(jnp.float32)
        pos_lo = (pos % 64).astype(jnp.float32)
        hi_iota = lax.broadcasted_iota(jnp.int32, (highs, total), 0).astype(jnp.float32)
        lo_iota = lax.broadcasted_iota(jnp.int32, (LOW, total), 0).astype(jnp.float32)
        slot_iota = (lax.broadcasted_iota(jnp.int32, (highs, LOW), 0) * LOW
                     + lax.broadcasted_iota(jnp.int32, (highs, LOW), 1)).astype(jnp.float32)
        for e in range(num_e):
            rank = rank_ref[e:e + 1, 0:total]
            gate = g_ref[e:e + 1, 0:total]
            hi = jnp.floor(rank * (1.0 / LOW))
            lo = rank - hi * LOW
            in_hi = hi_iota == hi
            in_lo = (lo_iota == lo).astype(jnp.float32).astype(jnp.bfloat16)
            gate_a = gate.astype(jnp.bfloat16).astype(jnp.float32)
            rest = gate - gate_a
            gate_b = rest.astype(jnp.bfloat16).astype(jnp.float32)
            gate_c = rest - gate_b
            left = jnp.concatenate(
                [jnp.where(in_hi, v, 0.0) for v in (pos_hi, pos_lo, gate_a, gate_b, gate_c)], axis=0)
            table = lax.dot_general(left.astype(jnp.bfloat16), in_lo, (((1,), (1,)), ((), ())),
                                    preferred_element_type=jnp.float32)
            tok = table[0:highs] * 64.0 + table[highs:2 * highs]
            live = slot_iota < carry[e:e + 1, 0:1]
            tok_ref[c, e] = jnp.where(live, tok, float(total)).astype(jnp.int32)
            gate_ref[c, e] = table[2 * highs:3 * highs] + (table[3 * highs:4 * highs] + table[4 * highs:5 * highs])
        tok_ref[c, num_e] = jnp.full((highs, LOW), total, jnp.int32)
        gate_ref[c, num_e] = jnp.zeros((highs, LOW), jnp.float32)
        start += size


def route(meta_all, me, sizes, top_k, num_e, rows_max):
    num_src = meta_all.shape[0]
    n_chunks = len(sizes)
    highs = rows_max // LOW
    width = num_src * max(sizes)
    tok, gate, cnt = pl.pallas_call(
        functools.partial(router_kernel, sizes, top_k),
        out_shape=(jax.ShapeDtypeStruct((n_chunks, num_e + 1, highs, LOW), jnp.int32),
                   jax.ShapeDtypeStruct((n_chunks, num_e + 1, highs, LOW), jnp.float32),
                   jax.ShapeDtypeStruct((n_chunks, num_e, LANES), jnp.int32)),
        in_specs=[pl.BlockSpec(memory_space=pltpu.VMEM), pl.BlockSpec(memory_space=pltpu.SMEM)],
        out_specs=(pl.BlockSpec(memory_space=pltpu.VMEM),) * 3,
        scratch_shapes=[pltpu.VMEM((num_e, width), jnp.float32), pltpu.VMEM((num_e, width), jnp.float32)],
        compiler_params=pltpu.CompilerParams(vmem_limit_bytes=32 * 1024 * 1024),
        name="router",
    )(meta_all, me)
    return (tok.reshape(n_chunks, num_e + 1, rows_max), gate.reshape(n_chunks, num_e + 1, rows_max), cnt[:, :, 0])


def ffn_kernel(cnt_ref, tok_ref, gate_ref, x_hbm, w1_hbm, w3_hbm, w2_hbm, out_hbm,
               stage, xf, yf, w1b, w3b, w2b, xg, xb, hb, rg, tile_e, tile_b, in_sem, w_sem, out_sem):
    num_e, hidden, ff = w1_hbm.shape
    rows = x_hbm.shape[0]
    piece = stage.shape[1]
    pieces = rows // piece
    groups = TILE // 8

    def weights(e):
        slot = lax.rem(e, 2)
        return [pltpu.make_async_copy(src.at[e], dst.at[slot], w_sem.at[slot, i])
                for i, (src, dst) in enumerate(((w1_hbm, w1b), (w3_hbm, w3b), (w2_hbm, w2b)))]

    def fetch(i, slot):
        return pltpu.make_async_copy(x_hbm.at[pl.ds(i * piece, piece), :], stage.at[slot], in_sem.at[slot])

    fetch(0, 0).start()
    for copy in weights(0):
        copy.start()
    fetch(1, 1).start()

    tile_e[0] = num_e
    tile_b[0] = 0

    def list_expert(e, g):
        def list_tile(i, g):
            tile_e[g] = e
            tile_b[g] = i * TILE
            return g + 1
        return lax.fori_loop(0, (cnt_ref[e] + TILE - 1) // TILE, list_tile, g)
    end = lax.fori_loop(0, num_e, list_expert, 1)
    tile_e[end] = num_e
    tile_b[end] = 0

    def take_piece(i, c):
        slot = lax.rem(i, 2)
        fetch(i, slot).wait()
        row0 = pl.multiple_of(i * piece, piece)
        xf[pl.ds(row0, piece), :] = stage[slot].astype(jnp.float32)
        yf[pl.ds(row0, piece), :] = jnp.zeros((piece, hidden), jnp.float32)

        @pl.when(i + 2 < pieces)
        def _():
            fetch(i + 2, slot).start()
        return c
    lax.fori_loop(0, pieces, take_piece, 0)
    xf[rows:rows + 8, :] = jnp.zeros((8, hidden), jnp.float32)
    yf[rows:rows + 8, :] = jnp.zeros((8, hidden), jnp.float32)

    def gather(e, base, j):
        sub = lax.broadcasted_iota(jnp.int32, (8, hidden), 0)
        out = jnp.broadcast_to(xf[pl.ds(tok_ref[e, base], 1), :], (8, hidden))
        for r in range(1, 8):
            row = xf[pl.ds(tok_ref[e, base + r], 1), :]
            out = jnp.where(sub == r, jnp.broadcast_to(row, (8, hidden)), out)
        xg[j * 8:j * 8 + 8, :] = out

    def combine(e, base, j):
        toks = [tok_ref[e, base + r] for r in range(8)]
        gates = [gate_ref[e, base + r] for r in range(8)]
        new = [yf[pl.ds(toks[r], 1), :] + gates[r] * rg[j * 8 + r:j * 8 + r + 1, :] for r in range(8)]
        for r in range(8):
            yf[pl.ds(toks[r], 1), :] = new[r]

    for j in range(groups):
        gather(tile_e[1], tile_b[1] + j * 8, j)

    def advance(e, c):
        for copy in weights(e):
            copy.wait()

        @pl.when(e + 1 < num_e)
        def _():
            for copy in weights(e + 1):
                copy.start()
        return c

    f_starts = list(range(0, ff, 256))
    d_step = 512
    d_starts = list(range(0, hidden, d_step))

    def one_tile(g, last_e):
        e = tile_e[g]
        lax.fori_loop(last_e + 1, e + 1, advance, 0)
        slot = lax.rem(e, 2)
        prev_e, prev_b = tile_e[g - 1], tile_b[g - 1]
        next_e, next_b = tile_e[g + 1], tile_b[g + 1]
        xb[...] = xg[...].astype(jnp.bfloat16)
        done = 0
        for i, f in enumerate(f_starts):
            stop = min(f + 256, ff)
            a = jnp.dot(xb[...], w1b[slot, :, f:stop], preferred_element_type=jnp.float32)
            b = jnp.dot(xb[...], w3b[slot, :, f:stop], preferred_element_type=jnp.float32)
            hb[:, f:stop] = (jax.nn.silu(a) * b).astype(jnp.bfloat16)
            goal = groups * (i + 1) // len(f_starts)
            for j in range(done, goal):
                combine(prev_e, prev_b + j * 8, j)
            done = goal
        done = 0
        for i, d in enumerate(d_starts):
            r = jnp.dot(hb[...], w2b[slot, :, d:d + d_step], preferred_element_type=jnp.float32)
            rg[:, d:d + d_step] = r.astype(jnp.bfloat16).astype(jnp.float32)
            goal = groups * (i + 1) // len(d_starts)
            for j in range(done, goal):
                gather(next_e, next_b + j * 8, j)
            done = goal
        return e

    last = lax.fori_loop(1, end, one_tile, -1)
    lax.fori_loop(last + 1, num_e, advance, 0)

    @pl.when(end > 1)
    def _():
        for j in range(groups):
            combine(tile_e[end - 1], tile_b[end - 1] + j * 8, j)

    copy = pltpu.make_async_copy(yf.at[pl.ds(0, rows), :], out_hbm, out_sem)
    copy.start()
    copy.wait()


def expert_ffn(cnt, tok, gate, x, w1, w3, w2):
    rows, hidden = x.shape
    num_e, _, ff = w1.shape
    piece = 128
    any_spec = pl.BlockSpec(memory_space=pl.ANY)
    smem_spec = pl.BlockSpec(memory_space=pltpu.SMEM)
    max_tiles = num_e * (tok.shape[1] // TILE) + 2
    return pl.pallas_call(
        ffn_kernel,
        out_shape=jax.ShapeDtypeStruct((rows, hidden), jnp.float32),
        in_specs=[smem_spec] * 3 + [any_spec] * 4,
        out_specs=any_spec,
        scratch_shapes=[pltpu.VMEM((2, piece, hidden), jnp.bfloat16),
                        pltpu.VMEM((rows + 8, hidden), jnp.float32),
                        pltpu.VMEM((rows + 8, hidden), jnp.float32),
                        pltpu.VMEM((2, hidden, ff), jnp.bfloat16),
                        pltpu.VMEM((2, hidden, ff), jnp.bfloat16),
                        pltpu.VMEM((2, ff, hidden), jnp.bfloat16),
                        pltpu.VMEM((TILE, hidden), jnp.float32),
                        pltpu.VMEM((TILE, hidden), jnp.bfloat16),
                        pltpu.VMEM((TILE, ff), jnp.bfloat16),
                        pltpu.VMEM((TILE, hidden), jnp.float32),
                        pltpu.SMEM((max_tiles,), jnp.int32),
                        pltpu.SMEM((max_tiles,), jnp.int32),
                        pltpu.SemaphoreType.DMA((2,)),
                        pltpu.SemaphoreType.DMA((2, 3)),
                        pltpu.SemaphoreType.DMA],
        compiler_params=pltpu.CompilerParams(vmem_limit_bytes=VMEM_BYTES),
        cost_estimate=pl.CostEstimate(flops=6 * rows * hidden * ff, bytes_accessed=6 * num_e * hidden * ff,
                                      transcendentals=0),
        name="expert_ffn",
    )(cnt, tok, gate, x, w1, w3, w2)


def solution(mesh):
    num_ep = mesh.shape['ep']
    row_spec = P(('dp', 'ep'), None)
    replicated = P()
    expert_spec = P('ep', None, None)

    def device_step(tokens, expert_ids, gate_vals, slots, shared_w1, shared_w3, shared_w2, shared_gate, expert_w1, expert_w3, expert_w2):
        tok_count, hidden = tokens.shape
        top_k = expert_ids.shape[1]
        num_e = expert_w1.shape[0]
        num_experts = num_e * num_ep
        capacity = 8 * ((2 * tok_count * top_k + 8 * num_experts - 1) // (8 * num_experts))
        rows_max = num_ep * capacity
        sizes = chunk_sizes(tok_count)
        me = lax.axis_index('ep').astype(jnp.int32).reshape(1)

        kept_ids = jnp.where(slots >= 0, expert_ids, -1).astype(jnp.float32)
        meta = jnp.concatenate([kept_ids, gate_vals], axis=1).T
        meta = jnp.pad(meta, ((0, -meta.shape[0] % 8), (0, 0)))
        meta_all = lax.all_gather(meta, 'ep', axis=0, tiled=False)
        tok, gate, cnt = route(meta_all, me, sizes, top_k, num_e, rows_max)

        start = 0
        gathered = []
        for size in sizes:
            x = lax.all_gather(tokens[start:start + size], 'ep', axis=0, tiled=False)
            gathered.append(x.reshape(num_ep * size, hidden))
            start += size

        gate_logit = jnp.dot(tokens, shared_gate, preferred_element_type=jnp.float32)
        shared_a = jnp.dot(tokens, shared_w1, preferred_element_type=jnp.float32)
        shared_b = jnp.dot(tokens, shared_w3, preferred_element_type=jnp.float32)
        shared_h = (jax.nn.silu(shared_a) * shared_b).astype(jnp.bfloat16)
        shared_out = jnp.dot(shared_h, shared_w2, preferred_element_type=jnp.float32)
        base = tokens.astype(jnp.float32) + jax.nn.sigmoid(gate_logit)[:, None] * shared_out

        parts = []
        start = 0
        for c, size in enumerate(sizes):
            partial = expert_ffn(cnt[c], tok[c], gate[c], gathered[c], expert_w1, expert_w3, expert_w2)
            routed = lax.psum_scatter(partial.reshape(num_ep, size, hidden), 'ep', scatter_dimension=0, tiled=False)
            parts.append((base[start:start + size] + routed).astype(jnp.bfloat16))
            start += size
        return jnp.concatenate(parts, axis=0)

    return jax.shard_map(device_step, mesh=mesh, in_specs=(row_spec, row_spec, row_spec, row_spec, replicated, replicated, replicated, replicated, expert_spec, expert_spec, expert_spec), out_specs=row_spec, check_vma=False)
```

```python
import functools

import jax
import jax.numpy as jnp
from jax import lax
from jax.experimental import pallas as pl
from jax.experimental.pallas import tpu as pltpu
from jax.sharding import PartitionSpec as P

LANES = 128
STEP = 64
TILE = 128
LOW = 32
PITCH = 24
VMEM_BYTES = 67043328


def chunk_sizes(tok_count):
    quarter = tok_count // 4
    rest = (tok_count - quarter) // 2
    return (quarter, rest, rest)


def router_kernel(sizes, top_k, meta_ref, me_ref, tok_ref, gate_ref, cnt_ref, rank_ref, g_ref):
    num_src = meta_ref.shape[0]
    num_e = rank_ref.shape[0]
    highs = tok_ref.shape[2]
    first = (me_ref[0] * num_e).astype(jnp.float32)
    e_idx = lax.broadcasted_iota(jnp.int32, (num_e, STEP), 0).astype(jnp.float32) + first
    upper = (lax.broadcasted_iota(jnp.int32, (STEP, STEP), 0)
             < lax.broadcasted_iota(jnp.int32, (STEP, STEP), 1)).astype(jnp.float32).astype(jnp.bfloat16)
    start = 0
    for c, size in enumerate(sizes):
        total = num_src * size
        carry = jnp.zeros((num_e, 1), jnp.float32)
        for s in range(num_src):
            for b in range(size // STEP):
                lane0 = start + b * STEP
                mask = jnp.zeros((num_e, STEP), jnp.float32)
                gate = jnp.zeros((num_e, STEP), jnp.float32)
                for k in range(top_k):
                    hit = meta_ref[s, k:k + 1, lane0:lane0 + STEP] == e_idx
                    mask = mask + jnp.where(hit, 1.0, 0.0)
                    gate = gate + jnp.where(hit, meta_ref[s, top_k + k:top_k + k + 1, lane0:lane0 + STEP], 0.0)
                rank = jnp.dot(mask.astype(jnp.bfloat16), upper, preferred_element_type=jnp.float32) + carry
                carry = carry + jnp.sum(mask, axis=1, keepdims=True)
                col = s * size + b * STEP
                rank_ref[:, col:col + STEP] = jnp.where(mask > 0.5, rank, -1.0)
                g_ref[:, col:col + STEP] = gate
        cnt_ref[c] = jnp.broadcast_to(carry, (num_e, LANES)).astype(jnp.int32)
        pos = lax.broadcasted_iota(jnp.int32, (1, total), 1)
        pos_hi = (pos // 64).astype(jnp.float32)
        pos_lo = (pos % 64).astype(jnp.float32)
        hi_iota = lax.broadcasted_iota(jnp.int32, (highs, total), 0).astype(jnp.float32)
        lo_iota = lax.broadcasted_iota(jnp.int32, (LOW, total), 0).astype(jnp.float32)
        slot_iota = (lax.broadcasted_iota(jnp.int32, (highs, LOW), 0) * LOW
                     + lax.broadcasted_iota(jnp.int32, (highs, LOW), 1)).astype(jnp.float32)
        for e in range(num_e):
            rank = rank_ref[e:e + 1, 0:total]
            gate = g_ref[e:e + 1, 0:total]
            hi = jnp.floor(rank * (1.0 / LOW))
            lo = rank - hi * LOW
            in_hi = hi_iota == hi
            in_lo = (lo_iota == lo).astype(jnp.float32).astype(jnp.bfloat16)
            gate_a = gate.astype(jnp.bfloat16).astype(jnp.float32)
            rest = gate - gate_a
            gate_b = rest.astype(jnp.bfloat16).astype(jnp.float32)
            gate_c = rest - gate_b
            left = jnp.concatenate(
                [jnp.where(in_hi, v, 0.0) for v in (pos_hi, pos_lo, gate_a, gate_b, gate_c)], axis=0)
            table = lax.dot_general(left.astype(jnp.bfloat16), in_lo, (((1,), (1,)), ((), ())),
                                    preferred_element_type=jnp.float32)
            tok = table[0:highs] * 64.0 + table[highs:2 * highs]
            live = slot_iota < carry[e:e + 1, 0:1]
            tok_ref[c, e] = jnp.where(live, tok, float(total)).astype(jnp.int32)
            gate_ref[c, e] = table[2 * highs:3 * highs] + (table[3 * highs:4 * highs] + table[4 * highs:5 * highs])
        tok_ref[c, num_e] = jnp.full((highs, LOW), total, jnp.int32)
        gate_ref[c, num_e] = jnp.zeros((highs, LOW), jnp.float32)
        start += size


def route(meta_all, me, sizes, top_k, num_e, rows_max):
    num_src = meta_all.shape[0]
    n_chunks = len(sizes)
    highs = rows_max // LOW
    width = num_src * max(sizes)
    tok, gate, cnt = pl.pallas_call(
        functools.partial(router_kernel, sizes, top_k),
        out_shape=(jax.ShapeDtypeStruct((n_chunks, num_e + 1, highs, LOW), jnp.int32),
                   jax.ShapeDtypeStruct((n_chunks, num_e + 1, highs, LOW), jnp.float32),
                   jax.ShapeDtypeStruct((n_chunks, num_e, LANES), jnp.int32)),
        in_specs=[pl.BlockSpec(memory_space=pltpu.VMEM), pl.BlockSpec(memory_space=pltpu.SMEM)],
        out_specs=(pl.BlockSpec(memory_space=pltpu.VMEM),) * 3,
        scratch_shapes=[pltpu.VMEM((num_e, width), jnp.float32), pltpu.VMEM((num_e, width), jnp.float32)],
        compiler_params=pltpu.CompilerParams(vmem_limit_bytes=32 * 1024 * 1024),
        name="router",
    )(meta_all, me)
    return (tok.reshape(n_chunks, -1), gate.reshape(n_chunks, -1), cnt[:, :, 0])


def ffn_kernel(cnt_ref, tok_ref, gate_ref, x_hbm, w1_hbm, w3_hbm, w2_hbm, out_hbm,
               xv, yf, w1b, w3b, w2b, xg, xb, hb, rg, tile_e, tile_b, in_sem, w_sem, out_sem):
    num_e, hidden, ff = w1_hbm.shape
    rows, subs, _ = x_hbm.shape
    groups = TILE // 8

    def weights(e):
        slot = lax.rem(e, 2)
        return [pltpu.make_async_copy(src.at[e], dst.at[slot], w_sem.at[slot, i])
                for i, (src, dst) in enumerate(((w1_hbm, w1b), (w3_hbm, w3b), (w2_hbm, w2b)))]

    def start_weights(e):
        for copy in weights(e):
            copy.start()

    fetch = pltpu.make_async_copy(x_hbm, xv.at[pl.ds(0, rows)], in_sem)
    fetch.start()
    start_weights(0)
    start_weights(1)

    rows_max = tok_ref.shape[0] // (num_e + 1)
    tile_e[0] = num_e
    tile_b[0] = num_e * rows_max

    def list_expert(e, g):
        def list_tile(i, g):
            tile_e[g] = e
            tile_b[g] = e * rows_max + i * TILE
            return g + 1
        return lax.fori_loop(0, (cnt_ref[e] + TILE - 1) // TILE, list_tile, g)
    end = lax.fori_loop(0, num_e, list_expert, 1)
    tile_e[end] = num_e
    tile_b[end] = num_e * rows_max

    def clear(i, c):
        yf[pl.ds(i * 32, 32)] = jnp.zeros((32, subs, LANES), jnp.float32)
        return c
    lax.fori_loop(0, rows // 32, clear, 0)
    yf[rows] = jnp.zeros((subs, LANES), jnp.float32)
    xv[rows] = jnp.zeros((subs, LANES), jnp.bfloat16)
    fetch.wait()

    def gather(base, i):
        xg[i * PITCH:i * PITCH + subs, :] = xv[tok_ref[base + i]].astype(jnp.float32)

    def pack(j):
        xb[:, j * LANES:(j + 1) * LANES] = xg[pl.ds(j, TILE, stride=PITCH), :].astype(jnp.bfloat16)

    def combine(base, j):
        toks = [tok_ref[base + j * 8 + r] for r in range(8)]
        gates = [gate_ref[base + j * 8 + r] for r in range(8)]
        new = []
        for r in range(8):
            at = (j * 8 + r) * PITCH
            new.append(yf[toks[r]] + gates[r] * rg[at:at + subs, :])
        for r in range(8):
            yf[toks[r]] = new[r]

    for i in range(TILE):
        gather(tile_b[1], i)
    for j in range(subs):
        pack(j)

    def advance(e, c):
        for copy in weights(e):
            copy.wait()

        @pl.when((cnt_ref[e] == 0) & (e + 2 < num_e))
        def _():
            start_weights(e + 2)
        return c

    f_starts = list(range(0, ff, 256))
    d_step = 512
    d_starts = list(range(0, hidden, d_step))

    def one_tile(g, last_e):
        e = tile_e[g]
        lax.fori_loop(last_e + 1, e + 1, advance, 0)
        slot = lax.rem(e, 2)
        prev_b = tile_b[g - 1]
        next_e, next_b = tile_e[g + 1], tile_b[g + 1]
        done = 0
        for i, f in enumerate(f_starts):
            stop = min(f + 256, ff)
            a = jnp.dot(xb[...], w1b[slot, :, f:stop], preferred_element_type=jnp.float32)
            b = jnp.dot(xb[...], w3b[slot, :, f:stop], preferred_element_type=jnp.float32)
            hb[:, f:stop] = (jax.nn.silu(a) * b).astype(jnp.bfloat16)
            goal = groups * (i + 1) // len(f_starts)
            for j in range(done, goal):
                combine(prev_b, j)
            done = goal
        for i in range(TILE):
            gather(next_b, i)
        for d in d_starts:
            r = jnp.dot(hb[...], w2b[slot, :, d:d + d_step], preferred_element_type=jnp.float32)
            r = r.astype(jnp.bfloat16).astype(jnp.float32)
            for j in range(d_step // LANES):
                rg[pl.ds(d // LANES + j, TILE, stride=PITCH), :] = r[:, j * LANES:(j + 1) * LANES]
        for j in range(subs):
            pack(j)

        @pl.when((next_e > e) & (e + 2 < num_e))
        def _():
            start_weights(e + 2)
        return e

    last = lax.fori_loop(1, end, one_tile, -1)
    lax.fori_loop(last + 1, num_e, advance, 0)

    @pl.when(end > 1)
    def _():
        for j in range(groups):
            combine(tile_b[end - 1], j)

    copy = pltpu.make_async_copy(yf.at[pl.ds(0, rows)], out_hbm, out_sem)
    copy.start()
    copy.wait()


def expert_ffn(cnt, tok, gate, x, w1, w3, w2):
    rows, subs, _ = x.shape
    num_e, hidden, ff = w1.shape
    any_spec = pl.BlockSpec(memory_space=pl.ANY)
    smem_spec = pl.BlockSpec(memory_space=pltpu.SMEM)
    max_tiles = tok.shape[0] // TILE + 2
    return pl.pallas_call(
        ffn_kernel,
        out_shape=jax.ShapeDtypeStruct((rows, subs, LANES), jnp.float32),
        in_specs=[smem_spec] * 3 + [any_spec] * 4,
        out_specs=any_spec,
        scratch_shapes=[pltpu.VMEM((rows + 1, subs, LANES), jnp.bfloat16),
                        pltpu.VMEM((rows + 1, subs, LANES), jnp.float32),
                        pltpu.VMEM((2, hidden, ff), jnp.bfloat16),
                        pltpu.VMEM((2, hidden, ff), jnp.bfloat16),
                        pltpu.VMEM((2, ff, hidden), jnp.bfloat16),
                        pltpu.VMEM((TILE * PITCH, LANES), jnp.float32),
                        pltpu.VMEM((TILE, hidden), jnp.bfloat16),
                        pltpu.VMEM((TILE, ff), jnp.bfloat16),
                        pltpu.VMEM((TILE * PITCH, LANES), jnp.float32),
                        pltpu.SMEM((max_tiles,), jnp.int32),
                        pltpu.SMEM((max_tiles,), jnp.int32),
                        pltpu.SemaphoreType.DMA,
                        pltpu.SemaphoreType.DMA((2, 3)),
                        pltpu.SemaphoreType.DMA],
        compiler_params=pltpu.CompilerParams(vmem_limit_bytes=VMEM_BYTES),
        cost_estimate=pl.CostEstimate(flops=6 * rows * hidden * ff, bytes_accessed=6 * num_e * hidden * ff,
                                      transcendentals=0),
        name="expert_ffn",
    )(cnt, tok, gate, x, w1, w3, w2)


def solution(mesh):
    num_ep = mesh.shape['ep']
    row_spec = P(('dp', 'ep'), None)
    replicated = P()
    expert_spec = P('ep', None, None)

    def device_step(tokens, expert_ids, gate_vals, slots, shared_w1, shared_w3, shared_w2, shared_gate, expert_w1, expert_w3, expert_w2):
        tok_count, hidden = tokens.shape
        top_k = expert_ids.shape[1]
        num_e = expert_w1.shape[0]
        num_experts = num_e * num_ep
        capacity = 8 * ((2 * tok_count * top_k + 8 * num_experts - 1) // (8 * num_experts))
        rows_max = num_ep * capacity
        sizes = chunk_sizes(tok_count)
        me = lax.axis_index('ep').astype(jnp.int32).reshape(1)

        kept_ids = jnp.where(slots >= 0, expert_ids, -1).astype(jnp.float32)
        meta = jnp.concatenate([kept_ids, gate_vals], axis=1).T
        meta = jnp.pad(meta, ((0, -meta.shape[0] % 8), (0, 0)))
        meta_all = lax.all_gather(meta, 'ep', axis=0, tiled=False)
        tok, gate, cnt = route(meta_all, me, sizes, top_k, num_e, rows_max)

        start = 0
        subs = hidden // LANES
        tokens3 = tokens.reshape(tok_count, subs, LANES)
        gathered = []
        for size in sizes:
            x = lax.all_gather(tokens3[start:start + size], 'ep', axis=0, tiled=False)
            gathered.append(x.reshape(num_ep * size, subs, LANES))
            start += size

        gate_logit = jnp.dot(tokens, shared_gate, preferred_element_type=jnp.float32)
        shared_a = jnp.dot(tokens, shared_w1, preferred_element_type=jnp.float32)
        shared_b = jnp.dot(tokens, shared_w3, preferred_element_type=jnp.float32)
        shared_h = (jax.nn.silu(shared_a) * shared_b).astype(jnp.bfloat16)
        shared_out = jnp.dot(shared_h, shared_w2, preferred_element_type=jnp.float32)
        base = tokens.astype(jnp.float32) + jax.nn.sigmoid(gate_logit)[:, None] * shared_out

        parts = []
        start = 0
        for c, size in enumerate(sizes):
            partial = expert_ffn(cnt[c], tok[c], gate[c], gathered[c], expert_w1, expert_w3, expert_w2)
            routed = lax.psum_scatter(partial.reshape(num_ep, size, subs, LANES), 'ep', scatter_dimension=0, tiled=False)
            parts.append((base[start:start + size] + routed.reshape(size, hidden)).astype(jnp.bfloat16))
            start += size
        return jnp.concatenate(parts, axis=0)

    return jax.shard_map(device_step, mesh=mesh, in_specs=(row_spec, row_spec, row_spec, row_spec, replicated, replicated, replicated, replicated, expert_spec, expert_spec, expert_spec), out_specs=row_spec, check_vma=False)
```

```python
import functools

import jax
import jax.numpy as jnp
from jax import lax
from jax.experimental import pallas as pl
from jax.experimental.pallas import tpu as pltpu
from jax.sharding import PartitionSpec as P

LANES = 128
STEP = 64
TILE = 128
LOW = 32
PITCH = 24
VMEM_BYTES = 67043328


def chunk_sizes(tok_count):
    quarter = tok_count // 4
    rest = (tok_count - quarter) // 2
    return (rest, rest, quarter)


def router_kernel(sizes, top_k, meta_ref, me_ref, tok_ref, gate_ref, cnt_ref, rank_ref, g_ref):
    num_src = meta_ref.shape[0]
    num_e = rank_ref.shape[0]
    highs = tok_ref.shape[2]
    first = (me_ref[0] * num_e).astype(jnp.float32)
    e_idx = lax.broadcasted_iota(jnp.int32, (num_e, STEP), 0).astype(jnp.float32) + first
    upper = (lax.broadcasted_iota(jnp.int32, (STEP, STEP), 0)
             < lax.broadcasted_iota(jnp.int32, (STEP, STEP), 1)).astype(jnp.float32).astype(jnp.bfloat16)
    start = 0
    for c, size in enumerate(sizes):
        total = num_src * size
        carry = jnp.zeros((num_e, 1), jnp.float32)
        for s in range(num_src):
            for b in range(size // STEP):
                lane0 = start + b * STEP
                mask = jnp.zeros((num_e, STEP), jnp.float32)
                gate = jnp.zeros((num_e, STEP), jnp.float32)
                for k in range(top_k):
                    hit = meta_ref[s, k:k + 1, lane0:lane0 + STEP] == e_idx
                    mask = mask + jnp.where(hit, 1.0, 0.0)
                    gate = gate + jnp.where(hit, meta_ref[s, top_k + k:top_k + k + 1, lane0:lane0 + STEP], 0.0)
                rank = jnp.dot(mask.astype(jnp.bfloat16), upper, preferred_element_type=jnp.float32) + carry
                carry = carry + jnp.sum(mask, axis=1, keepdims=True)
                col = s * size + b * STEP
                rank_ref[:, col:col + STEP] = jnp.where(mask > 0.5, rank, -1.0)
                g_ref[:, col:col + STEP] = gate
        cnt_ref[c] = jnp.broadcast_to(carry, (num_e, LANES)).astype(jnp.int32)
        pos = lax.broadcasted_iota(jnp.int32, (1, total), 1)
        pos_hi = (pos // 64).astype(jnp.float32)
        pos_lo = (pos % 64).astype(jnp.float32)
        hi_iota = lax.broadcasted_iota(jnp.int32, (highs, total), 0).astype(jnp.float32)
        lo_iota = lax.broadcasted_iota(jnp.int32, (LOW, total), 0).astype(jnp.float32)
        slot_iota = (lax.broadcasted_iota(jnp.int32, (highs, LOW), 0) * LOW
                     + lax.broadcasted_iota(jnp.int32, (highs, LOW), 1)).astype(jnp.float32)
        for e in range(num_e):
            rank = rank_ref[e:e + 1, 0:total]
            gate = g_ref[e:e + 1, 0:total]
            hi = jnp.floor(rank * (1.0 / LOW))
            lo = rank - hi * LOW
            in_hi = hi_iota == hi
            in_lo = (lo_iota == lo).astype(jnp.float32).astype(jnp.bfloat16)
            gate_a = gate.astype(jnp.bfloat16).astype(jnp.float32)
            rest = gate - gate_a
            gate_b = rest.astype(jnp.bfloat16).astype(jnp.float32)
            gate_c = rest - gate_b
            left = jnp.concatenate(
                [jnp.where(in_hi, v, 0.0) for v in (pos_hi, pos_lo, gate_a, gate_b, gate_c)], axis=0)
            table = lax.dot_general(left.astype(jnp.bfloat16), in_lo, (((1,), (1,)), ((), ())),
                                    preferred_element_type=jnp.float32)
            tok = table[0:highs] * 64.0 + table[highs:2 * highs]
            live = slot_iota < carry[e:e + 1, 0:1]
            tok_ref[c, e] = jnp.where(live, tok, float(total)).astype(jnp.int32)
            gate_ref[c, e] = table[2 * highs:3 * highs] + (table[3 * highs:4 * highs] + table[4 * highs:5 * highs])
        tok_ref[c, num_e] = jnp.full((highs, LOW), total, jnp.int32)
        gate_ref[c, num_e] = jnp.zeros((highs, LOW), jnp.float32)
        start += size


def route(meta_all, me, sizes, top_k, num_e, rows_max):
    num_src = meta_all.shape[0]
    n_chunks = len(sizes)
    highs = rows_max // LOW
    width = num_src * max(sizes)
    tok, gate, cnt = pl.pallas_call(
        functools.partial(router_kernel, sizes, top_k),
        out_shape=(jax.ShapeDtypeStruct((n_chunks, num_e + 1, highs, LOW), jnp.int32),
                   jax.ShapeDtypeStruct((n_chunks, num_e + 1, highs, LOW), jnp.float32),
                   jax.ShapeDtypeStruct((n_chunks, num_e, LANES), jnp.int32)),
        in_specs=[pl.BlockSpec(memory_space=pltpu.VMEM), pl.BlockSpec(memory_space=pltpu.SMEM)],
        out_specs=(pl.BlockSpec(memory_space=pltpu.VMEM),) * 3,
        scratch_shapes=[pltpu.VMEM((num_e, width), jnp.float32), pltpu.VMEM((num_e, width), jnp.float32)],
        compiler_params=pltpu.CompilerParams(vmem_limit_bytes=32 * 1024 * 1024),
        name="router",
    )(meta_all, me)
    return (tok.reshape(n_chunks, -1), gate.reshape(n_chunks, -1), cnt[:, :, 0])


def ffn_kernel(cnt_ref, tok_ref, gate_ref, x_hbm, w1_hbm, w3_hbm, w2_hbm, out_hbm,
               xv, yf, w1b, w3b, w2b, xg, xb, hb, rg, tile_e, tile_b, in_sem, w_sem, out_sem):
    num_e, hidden, ff = w1_hbm.shape
    rows, subs, _ = x_hbm.shape
    groups = TILE // 8

    def weights(e):
        slot = lax.rem(e, 2)
        return [pltpu.make_async_copy(src.at[e], dst.at[slot], w_sem.at[slot, i])
                for i, (src, dst) in enumerate(((w1_hbm, w1b), (w3_hbm, w3b), (w2_hbm, w2b)))]

    def start_weights(e):
        for copy in weights(e):
            copy.start()

    fetch = pltpu.make_async_copy(x_hbm, xv.at[pl.ds(0, rows)], in_sem)
    fetch.start()
    start_weights(0)
    start_weights(1)

    rows_max = tok_ref.shape[0] // (num_e + 1)
    tile_e[0] = num_e
    tile_b[0] = num_e * rows_max

    def list_expert(e, g):
        def list_tile(i, g):
            tile_e[g] = e
            tile_b[g] = e * rows_max + i * TILE
            return g + 1
        return lax.fori_loop(0, (cnt_ref[e] + TILE - 1) // TILE, list_tile, g)
    end = lax.fori_loop(0, num_e, list_expert, 1)
    tile_e[end] = num_e
    tile_b[end] = num_e * rows_max

    def clear(i, c):
        yf[pl.ds(i * 32, 32)] = jnp.zeros((32, subs, LANES), jnp.float32)
        return c
    lax.fori_loop(0, rows // 32, clear, 0)
    yf[rows] = jnp.zeros((subs, LANES), jnp.float32)
    xv[rows] = jnp.zeros((subs, LANES), jnp.bfloat16)
    fetch.wait()

    def gather(base, i):
        xg[i * PITCH:i * PITCH + subs, :] = xv[tok_ref[base + i]].astype(jnp.float32)

    def pack(j):
        xb[:, j * LANES:(j + 1) * LANES] = xg[pl.ds(j, TILE, stride=PITCH), :].astype(jnp.bfloat16)

    def combine(base, j):
        toks = [tok_ref[base + j * 8 + r] for r in range(8)]
        gates = [gate_ref[base + j * 8 + r] for r in range(8)]
        new = []
        for r in range(8):
            at = (j * 8 + r) * PITCH
            new.append(yf[toks[r]] + gates[r] * rg[at:at + subs, :])
        for r in range(8):
            yf[toks[r]] = new[r]

    for i in range(TILE):
        gather(tile_b[1], i)
    for j in range(subs):
        pack(j)

    def advance(e, c):
        for copy in weights(e):
            copy.wait()

        @pl.when((cnt_ref[e] == 0) & (e + 2 < num_e))
        def _():
            start_weights(e + 2)
        return c

    f_starts = list(range(0, ff, 256))
    d_step = 512
    d_starts = list(range(0, hidden, d_step))

    def one_tile(g, last_e):
        e = tile_e[g]
        lax.fori_loop(last_e + 1, e + 1, advance, 0)
        slot = lax.rem(e, 2)
        prev_b = tile_b[g - 1]
        next_e, next_b = tile_e[g + 1], tile_b[g + 1]
        done = 0
        for i, f in enumerate(f_starts):
            stop = min(f + 256, ff)
            a = jnp.dot(xb[...], w1b[slot, :, f:stop], preferred_element_type=jnp.float32)
            b = jnp.dot(xb[...], w3b[slot, :, f:stop], preferred_element_type=jnp.float32)
            hb[:, f:stop] = (jax.nn.silu(a) * b).astype(jnp.bfloat16)
            goal = groups * (i + 1) // len(f_starts)
            for j in range(done, goal):
                combine(prev_b, j)
            done = goal
        for i in range(TILE):
            gather(next_b, i)
        for d in d_starts:
            r = jnp.dot(hb[...], w2b[slot, :, d:d + d_step], preferred_element_type=jnp.float32)
            r = r.astype(jnp.bfloat16).astype(jnp.float32)
            for j in range(d_step // LANES):
                rg[pl.ds(d // LANES + j, TILE, stride=PITCH), :] = r[:, j * LANES:(j + 1) * LANES]
        for j in range(subs):
            pack(j)

        @pl.when((next_e > e) & (e + 2 < num_e))
        def _():
            start_weights(e + 2)
        return e

    last = lax.fori_loop(1, end, one_tile, -1)
    lax.fori_loop(last + 1, num_e, advance, 0)

    @pl.when(end > 1)
    def _():
        for j in range(groups):
            combine(tile_b[end - 1], j)

    copy = pltpu.make_async_copy(yf.at[pl.ds(0, rows)], out_hbm, out_sem)
    copy.start()
    copy.wait()


def expert_ffn(cnt, tok, gate, x, w1, w3, w2):
    rows, subs, _ = x.shape
    num_e, hidden, ff = w1.shape
    any_spec = pl.BlockSpec(memory_space=pl.ANY)
    smem_spec = pl.BlockSpec(memory_space=pltpu.SMEM)
    max_tiles = tok.shape[0] // TILE + 2
    return pl.pallas_call(
        ffn_kernel,
        out_shape=jax.ShapeDtypeStruct((rows, subs, LANES), jnp.float32),
        in_specs=[smem_spec] * 3 + [any_spec] * 4,
        out_specs=any_spec,
        scratch_shapes=[pltpu.VMEM((rows + 1, subs, LANES), jnp.bfloat16),
                        pltpu.VMEM((rows + 1, subs, LANES), jnp.float32),
                        pltpu.VMEM((2, hidden, ff), jnp.bfloat16),
                        pltpu.VMEM((2, hidden, ff), jnp.bfloat16),
                        pltpu.VMEM((2, ff, hidden), jnp.bfloat16),
                        pltpu.VMEM((TILE * PITCH, LANES), jnp.float32),
                        pltpu.VMEM((TILE, hidden), jnp.bfloat16),
                        pltpu.VMEM((TILE, ff), jnp.bfloat16),
                        pltpu.VMEM((TILE * PITCH, LANES), jnp.float32),
                        pltpu.SMEM((max_tiles,), jnp.int32),
                        pltpu.SMEM((max_tiles,), jnp.int32),
                        pltpu.SemaphoreType.DMA,
                        pltpu.SemaphoreType.DMA((2, 3)),
                        pltpu.SemaphoreType.DMA],
        compiler_params=pltpu.CompilerParams(vmem_limit_bytes=VMEM_BYTES),
        cost_estimate=pl.CostEstimate(flops=6 * rows * hidden * ff, bytes_accessed=6 * num_e * hidden * ff,
                                      transcendentals=0),
        name="expert_ffn",
    )(cnt, tok, gate, x, w1, w3, w2)


def solution(mesh):
    num_ep = mesh.shape['ep']
    row_spec = P(('dp', 'ep'), None)
    replicated = P()
    expert_spec = P('ep', None, None)

    def device_step(tokens, expert_ids, gate_vals, slots, shared_w1, shared_w3, shared_w2, shared_gate, expert_w1, expert_w3, expert_w2):
        tok_count, hidden = tokens.shape
        top_k = expert_ids.shape[1]
        num_e = expert_w1.shape[0]
        num_experts = num_e * num_ep
        capacity = 8 * ((2 * tok_count * top_k + 8 * num_experts - 1) // (8 * num_experts))
        rows_max = num_ep * capacity
        sizes = chunk_sizes(tok_count)
        me = lax.axis_index('ep').astype(jnp.int32).reshape(1)

        kept_ids = jnp.where(slots >= 0, expert_ids, -1).astype(jnp.float32)
        meta = jnp.concatenate([kept_ids, gate_vals], axis=1).T
        meta = jnp.pad(meta, ((0, -meta.shape[0] % 8), (0, 0)))
        meta_all = lax.all_gather(meta, 'ep', axis=0, tiled=False)
        tok, gate, cnt = route(meta_all, me, sizes, top_k, num_e, rows_max)

        start = 0
        subs = hidden // LANES
        tokens3 = tokens.reshape(tok_count, subs, LANES)
        gathered = []
        for size in sizes:
            x = lax.all_gather(tokens3[start:start + size], 'ep', axis=0, tiled=False)
            gathered.append(x.reshape(num_ep * size, subs, LANES))
            start += size

        gate_logit = jnp.dot(tokens, shared_gate, preferred_element_type=jnp.float32)
        shared_a = jnp.dot(tokens, shared_w1, preferred_element_type=jnp.float32)
        shared_b = jnp.dot(tokens, shared_w3, preferred_element_type=jnp.float32)
        shared_h = (jax.nn.silu(shared_a) * shared_b).astype(jnp.bfloat16)
        shared_out = jnp.dot(shared_h, shared_w2, preferred_element_type=jnp.float32)
        base = tokens.astype(jnp.float32) + jax.nn.sigmoid(gate_logit)[:, None] * shared_out

        parts = []
        start = 0
        for c, size in enumerate(sizes):
            partial = expert_ffn(cnt[c], tok[c], gate[c], gathered[c], expert_w1, expert_w3, expert_w2)
            routed = lax.psum_scatter(partial.reshape(num_ep, size, subs, LANES), 'ep', scatter_dimension=0, tiled=False)
            parts.append((base[start:start + size] + routed.reshape(size, hidden)).astype(jnp.bfloat16))
            start += size
        return jnp.concatenate(parts, axis=0)

    return jax.shard_map(device_step, mesh=mesh, in_specs=(row_spec, row_spec, row_spec, row_spec, replicated, replicated, replicated, replicated, expert_spec, expert_spec, expert_spec), out_specs=row_spec, check_vma=False)
```

```python
import functools

import jax
import jax.numpy as jnp
from jax import lax
from jax.experimental import pallas as pl
from jax.experimental.pallas import tpu as pltpu
from jax.sharding import PartitionSpec as P


LANES = 128
STEP = 64
TILE = 128
LOW = 32
PITCH = 24
VMEM_BYTES = 67043328


def chunk_spans(tok_count):
    quarter = tok_count // 4
    rest = (tok_count - quarter) // 2
    return ((quarter + rest, rest), (quarter, rest), (0, quarter))


def router_kernel(spans, top_k, meta_ref, me_ref, tok_ref, gate_ref, cnt_ref, rank_ref, g_ref):
    num_src = meta_ref.shape[0]
    num_e = rank_ref.shape[0]
    highs = tok_ref.shape[2]
    first = (me_ref[0] * num_e).astype(jnp.float32)
    e_idx = lax.broadcasted_iota(jnp.int32, (num_e, STEP), 0).astype(jnp.float32) + first
    upper = (lax.broadcasted_iota(jnp.int32, (STEP, STEP), 0)
             < lax.broadcasted_iota(jnp.int32, (STEP, STEP), 1)).astype(jnp.float32).astype(jnp.bfloat16)
    for c, (start, size) in enumerate(spans):
        total = num_src * size
        carry = jnp.zeros((num_e, 1), jnp.float32)
        for s in range(num_src):
            for b in range(size // STEP):
                lane0 = start + b * STEP
                mask = jnp.zeros((num_e, STEP), jnp.float32)
                gate = jnp.zeros((num_e, STEP), jnp.float32)
                for k in range(top_k):
                    hit = meta_ref[s, k:k + 1, lane0:lane0 + STEP] == e_idx
                    mask = mask + jnp.where(hit, 1.0, 0.0)
                    gate = gate + jnp.where(hit, meta_ref[s, top_k + k:top_k + k + 1, lane0:lane0 + STEP], 0.0)
                rank = jnp.dot(mask.astype(jnp.bfloat16), upper, preferred_element_type=jnp.float32) + carry
                carry = carry + jnp.sum(mask, axis=1, keepdims=True)
                col = s * size + b * STEP
                rank_ref[:, col:col + STEP] = jnp.where(mask > 0.5, rank, -1.0)
                g_ref[:, col:col + STEP] = gate
        cnt_ref[c] = jnp.broadcast_to(carry, (num_e, LANES)).astype(jnp.int32)
        pos = lax.broadcasted_iota(jnp.int32, (1, total), 1)
        pos_hi = (pos // 64).astype(jnp.float32)
        pos_lo = (pos % 64).astype(jnp.float32)
        hi_iota = lax.broadcasted_iota(jnp.int32, (highs, total), 0).astype(jnp.float32)
        lo_iota = lax.broadcasted_iota(jnp.int32, (LOW, total), 0).astype(jnp.float32)
        slot_iota = (lax.broadcasted_iota(jnp.int32, (highs, LOW), 0) * LOW
                     + lax.broadcasted_iota(jnp.int32, (highs, LOW), 1)).astype(jnp.float32)
        for e in range(num_e):
            rank = rank_ref[e:e + 1, 0:total]
            gate = g_ref[e:e + 1, 0:total]
            hi = jnp.floor(rank * (1.0 / LOW))
            lo = rank - hi * LOW
            in_hi = hi_iota == hi
            in_lo = (lo_iota == lo).astype(jnp.float32).astype(jnp.bfloat16)
            gate_a = gate.astype(jnp.bfloat16).astype(jnp.float32)
            rest = gate - gate_a
            gate_b = rest.astype(jnp.bfloat16).astype(jnp.float32)
            gate_c = rest - gate_b
            left = jnp.concatenate(
                [jnp.where(in_hi, v, 0.0) for v in (pos_hi, pos_lo, gate_a, gate_b, gate_c)], axis=0)
            table = lax.dot_general(left.astype(jnp.bfloat16), in_lo, (((1,), (1,)), ((), ())),
                                    preferred_element_type=jnp.float32)
            tok = table[0:highs] * 64.0 + table[highs:2 * highs]
            live = slot_iota < carry[e:e + 1, 0:1]
            tok_ref[c, e] = jnp.where(live, tok, float(total)).astype(jnp.int32)
            gate_ref[c, e] = table[2 * highs:3 * highs] + (table[3 * highs:4 * highs] + table[4 * highs:5 * highs])
        tok_ref[c, num_e] = jnp.full((highs, LOW), total, jnp.int32)
        gate_ref[c, num_e] = jnp.zeros((highs, LOW), jnp.float32)


def route(meta_all, me, spans, top_k, num_e, rows_max):
    num_src = meta_all.shape[0]
    n_chunks = len(spans)
    highs = rows_max // LOW
    width = num_src * max(size for _, size in spans)
    tok, gate, cnt = pl.pallas_call(
        functools.partial(router_kernel, spans, top_k),
        out_shape=(jax.ShapeDtypeStruct((n_chunks, num_e + 1, highs, LOW), jnp.int32),
                   jax.ShapeDtypeStruct((n_chunks, num_e + 1, highs, LOW), jnp.float32),
                   jax.ShapeDtypeStruct((n_chunks, num_e, LANES), jnp.int32)),
        in_specs=[pl.BlockSpec(memory_space=pltpu.VMEM), pl.BlockSpec(memory_space=pltpu.SMEM)],
        out_specs=(pl.BlockSpec(memory_space=pltpu.VMEM),) * 3,
        scratch_shapes=[pltpu.VMEM((num_e, width), jnp.float32), pltpu.VMEM((num_e, width), jnp.float32)],
        compiler_params=pltpu.CompilerParams(vmem_limit_bytes=32 * 1024 * 1024),
        name="router",
    )(meta_all, me)
    return (tok.reshape(n_chunks, -1), gate.reshape(n_chunks, -1), cnt[:, :, 0])


def ffn_kernel(offset, size, cnt_ref, tok_ref, gate_ref, x_hbm, w1_hbm, w3_hbm, w2_hbm, out_hbm,
               xv, yf, w1b, w3b, w2b, xg, xb, hb, rg, tile_e, tile_b, in_sem, w_sem, out_sem):
    num_e, hidden, ff = w1_hbm.shape
    num_src, _, subs, _ = x_hbm.shape
    rows = num_src * size
    groups = TILE // 8

    def weights(e):
        slot = lax.rem(e, 2)
        return [pltpu.make_async_copy(src.at[e], dst.at[slot], w_sem.at[slot, i])
                for i, (src, dst) in enumerate(((w1_hbm, w1b), (w3_hbm, w3b), (w2_hbm, w2b)))]

    def start_weights(e):
        for copy in weights(e):
            copy.start()

    fetches = [pltpu.make_async_copy(x_hbm.at[i, pl.ds(offset, size)], xv.at[pl.ds(i * size, size)], in_sem.at[i])
               for i in range(num_src)]
    for fetch in fetches:
        fetch.start()
    start_weights(0)
    start_weights(1)

    rows_max = tok_ref.shape[0] // (num_e + 1)
    tile_e[0] = num_e
    tile_b[0] = num_e * rows_max

    def list_expert(e, g):
        def list_tile(i, g):
            tile_e[g] = e
            tile_b[g] = e * rows_max + i * TILE
            return g + 1

        return lax.fori_loop(0, (cnt_ref[e] + TILE - 1) // TILE, list_tile, g)

    end = lax.fori_loop(0, num_e, list_expert, 1)
    tile_e[end] = num_e
    tile_b[end] = num_e * rows_max

    def clear(i, c):
        yf[pl.ds(i * 32, 32)] = jnp.zeros((32, subs, LANES), jnp.float32)
        return c

    lax.fori_loop(0, rows // 32, clear, 0)
    yf[rows] = jnp.zeros((subs, LANES), jnp.float32)
    xv[rows] = jnp.zeros((subs, LANES), jnp.bfloat16)
    for fetch in fetches:
        fetch.wait()

    def gather(base, i):
        xg[i * PITCH:i * PITCH + subs, :] = xv[tok_ref[base + i]].astype(jnp.float32)

    def pack(j):
        xb[:, j * LANES:(j + 1) * LANES] = xg[pl.ds(j, TILE, stride=PITCH), :].astype(jnp.bfloat16)

    def combine(base, j):
        toks = [tok_ref[base + j * 8 + r] for r in range(8)]
        gates = [gate_ref[base + j * 8 + r] for r in range(8)]
        new = []
        for r in range(8):
            at = (j * 8 + r) * PITCH
            new.append(yf[toks[r]] + gates[r] * rg[at:at + subs, :])
        for r in range(8):
            yf[toks[r]] = new[r]

    for i in range(TILE):
        gather(tile_b[1], i)
    for j in range(subs):
        pack(j)

    def advance(e, c):
        for copy in weights(e):
            copy.wait()

        @pl.when((cnt_ref[e] == 0) & (e + 2 < num_e))
        def _():
            start_weights(e + 2)

        return c

    f_starts = list(range(0, ff, 256))
    d_step = 512
    d_starts = list(range(0, hidden, d_step))

    def one_tile(g, last_e):
        e = tile_e[g]
        lax.fori_loop(last_e + 1, e + 1, advance, 0)
        slot = lax.rem(e, 2)
        prev_b = tile_b[g - 1]
        next_e, next_b = tile_e[g + 1], tile_b[g + 1]
        done = 0
        for i, f in enumerate(f_starts):
            stop = min(f + 256, ff)
            a = jnp.dot(xb[...], w1b[slot, :, f:stop], preferred_element_type=jnp.float32)
            b = jnp.dot(xb[...], w3b[slot, :, f:stop], preferred_element_type=jnp.float32)
            hb[:, f:stop] = (jax.nn.silu(a) * b).astype(jnp.bfloat16)
            goal = groups * (i + 1) // len(f_starts)
            for j in range(done, goal):
                combine(prev_b, j)
            done = goal
        for i in range(TILE):
            gather(next_b, i)
        for d in d_starts:
            r = jnp.dot(hb[...], w2b[slot, :, d:d + d_step], preferred_element_type=jnp.float32)
            r = r.astype(jnp.bfloat16).astype(jnp.float32)
            for j in range(d_step // LANES):
                rg[pl.ds(d // LANES + j, TILE, stride=PITCH), :] = r[:, j * LANES:(j + 1) * LANES]
        for j in range(subs):
            pack(j)

        @pl.when((next_e > e) & (e + 2 < num_e))
        def _():
            start_weights(e + 2)

        return e

    last = lax.fori_loop(1, end, one_tile, -1)
    lax.fori_loop(last + 1, num_e, advance, 0)

    @pl.when(end > 1)
    def _():
        for j in range(groups):
            combine(tile_b[end - 1], j)

    copy = pltpu.make_async_copy(yf.at[pl.ds(0, rows)], out_hbm, out_sem)
    copy.start()
    copy.wait()


def expert_ffn(cnt, tok, gate, x, offset, size, w1, w3, w2):
    num_src, _, subs, _ = x.shape
    rows = num_src * size
    num_e, hidden, ff = w1.shape
    any_spec = pl.BlockSpec(memory_space=pl.ANY)
    smem_spec = pl.BlockSpec(memory_space=pltpu.SMEM)
    max_tiles = tok.shape[0] // TILE + 2
    return pl.pallas_call(
        functools.partial(ffn_kernel, offset, size),
        out_shape=jax.ShapeDtypeStruct((rows, subs, LANES), jnp.float32),
        in_specs=[smem_spec] * 3 + [any_spec] * 4,
        out_specs=any_spec,
        scratch_shapes=[pltpu.VMEM((rows + 1, subs, LANES), jnp.bfloat16),
                        pltpu.VMEM((rows + 1, subs, LANES), jnp.float32),
                        pltpu.VMEM((2, hidden, ff), jnp.bfloat16),
                        pltpu.VMEM((2, hidden, ff), jnp.bfloat16),
                        pltpu.VMEM((2, ff, hidden), jnp.bfloat16),
                        pltpu.VMEM((TILE * PITCH, LANES), jnp.float32),
                        pltpu.VMEM((TILE, hidden), jnp.bfloat16),
                        pltpu.VMEM((TILE, ff), jnp.bfloat16),
                        pltpu.VMEM((TILE * PITCH, LANES), jnp.float32),
                        pltpu.SMEM((max_tiles,), jnp.int32),
                        pltpu.SMEM((max_tiles,), jnp.int32),
                        pltpu.SemaphoreType.DMA((num_src,)),
                        pltpu.SemaphoreType.DMA((2, 3)),
                        pltpu.SemaphoreType.DMA],
        compiler_params=pltpu.CompilerParams(vmem_limit_bytes=VMEM_BYTES),
        cost_estimate=pl.CostEstimate(flops=6 * rows * hidden * ff, bytes_accessed=6 * num_e * hidden * ff,
                                      transcendentals=0),
        name="expert_ffn",
    )(cnt, tok, gate, x, w1, w3, w2)


def solution(mesh):
    num_ep = mesh.shape['ep']
    row_spec = P(('dp', 'ep'), None)
    replicated = P()
    expert_spec = P('ep', None, None)

    def device_step(tokens, expert_ids, gate_vals, slots, shared_w1, shared_w3, shared_w2, shared_gate, expert_w1, expert_w3, expert_w2):
        tok_count, hidden = tokens.shape
        top_k = expert_ids.shape[1]
        num_e = expert_w1.shape[0]
        num_experts = num_e * num_ep
        capacity = 8 * ((2 * tok_count * top_k + 8 * num_experts - 1) // (8 * num_experts))
        rows_max = num_ep * capacity
        spans = chunk_spans(tok_count)
        me = lax.axis_index('ep').astype(jnp.int32).reshape(1)

        kept_ids = jnp.where(slots >= 0, expert_ids, -1).astype(jnp.float32)
        meta = jnp.concatenate([kept_ids, gate_vals], axis=1).T
        meta = jnp.pad(meta, ((0, -meta.shape[0] % 8), (0, 0)))
        meta_all = lax.all_gather(meta, 'ep', axis=0, tiled=False)
        tok, gate, cnt = route(meta_all, me, spans, top_k, num_e, rows_max)

        subs = hidden // LANES
        tokens3 = tokens.reshape(tok_count, subs, LANES)
        first = spans[0][0]
        early = lax.all_gather(tokens3[first:], 'ep', axis=0, tiled=False)
        late = lax.all_gather(tokens3[:first], 'ep', axis=0, tiled=False)

        gate_logit = jnp.dot(tokens, shared_gate, preferred_element_type=jnp.float32)
        shared_a = jnp.dot(tokens, shared_w1, preferred_element_type=jnp.float32)
        shared_b = jnp.dot(tokens, shared_w3, preferred_element_type=jnp.float32)
        shared_h = (jax.nn.silu(shared_a) * shared_b).astype(jnp.bfloat16)
        shared_out = jnp.dot(shared_h, shared_w2, preferred_element_type=jnp.float32)
        base = tokens.astype(jnp.float32) + jax.nn.sigmoid(gate_logit)[:, None] * shared_out

        parts = []
        for c, (start, size) in enumerate(spans):
            x, offset = (early, 0) if c == 0 else (late, start)
            partial = expert_ffn(cnt[c], tok[c], gate[c], x, offset, size, expert_w1, expert_w3, expert_w2)
            routed = lax.psum_scatter(partial.reshape(num_ep, size, subs, LANES), 'ep', scatter_dimension=0, tiled=False)
            parts.append((base[start:start + size] + routed.reshape(size, hidden)).astype(jnp.bfloat16))
        out = jnp.concatenate([jnp.zeros_like(parts[2])] + parts[1::-1], axis=0)
        return lax.dynamic_update_slice(out, parts[2], (0, 0))

    return jax.shard_map(device_step, mesh=mesh, in_specs=(row_spec, row_spec, row_spec, row_spec, replicated, replicated, replicated, replicated, expert_spec, expert_spec, expert_spec), out_specs=row_spec, check_vma=False)
```
